512 devices in a mesh: grp: 2 (over y), gx: 32 (over z), gy: 4 (over x), gz: 2 (over core).
Axes of the slice: x: 4, y: 2, z: 32, core: 2. Of those that a mesh axis runs over, the one named last changes fastest.
The devices are a block of a 4x8x32 slice.
Arguments:
- position: float32 [64, 128, 8, 256], P(None, ('grp', 'gx'), 'gy', 'gz'), parts along dimension 1, may hold values from -6 to 6
- momentum: float32 [64, 128, 8, 256], P(None, ('grp', 'gx'), 'gy', 'gz'), parts along dimension 1, may hold values from -6 to 6
- noise: bfloat16 [3, 64, 128, 8, 256], P(None, None, ('grp', 'gx'), 'gy', 'gz'), parts along dimension 2, may hold values from -6 to 6
- filter_in: bfloat16 [64, 64, 3, 3, 3], P('gx', 'gy'), may hold values from -0.15625 to 0.15625
- filter_out: bfloat16 [64, 64, 3, 3, 3], P('gx', 'gy'), may hold values from -0.15625 to 0.15625
- bias: float32 [64], replicated, may hold values from -4 to 4
Outputs:
- final_position: float32 [64, 128, 8, 256], P(None, ('grp', 'gx'), 'gy', 'gz'), parts along dimension 1
- final_momentum: float32 [64, 128, 8, 256], P(None, ('grp', 'gx'), 'gy', 'gz'), parts along dimension 1
The draws below stay inside these ranges and needn't reach their ends.
There are 2 independent parts, one for each index of `grp`. The reference program is written for one: setup_inputs(seed, part) draws one part's arguments, and reference() takes and returns one part's arrays. A program takes and returns all parts, laid end to end along the dimension named above; an argument that names none is the same for every part. Nothing has to cross between parts.
All inputs are finite; a program needn't handle non-finite values.
Results may differ from the reference program's by a relative error of at most 0.0013.
Values may be sent and summed in bfloat16 or wider, within the bound.
A program may use at most 64 MiB of HBM per device.

```python
import jax
import jax.numpy as jnp
from jax import lax

C = 64
STEPS = 3
NX = 64
NY = 8
NZ = 256


def block_scale(own_key, shape, pieces, smallest, top_value):
    def one(axis_at, parts):
        steps = jax.random.uniform(jax.random.fold_in(jax.random.fold_in(own_key, 6), axis_at), (parts,), jnp.float32, smallest / len(pieces), top_value / len(pieces))
        return jnp.repeat(jnp.exp(steps), shape[axis_at] // parts).reshape((-1,) + (1,) * (len(shape) - axis_at - 1))

    loudness = one(*pieces[0])
    for cut in pieces[1:]:
        loudness = loudness * one(*cut)
    return loudness


def scatter_about(key, dims, scale, most, pieces=(), kind=jnp.bfloat16):
    drawn = jax.random.normal(key, dims, jnp.float32) * scale
    if len(pieces) > 0:
        drawn = block_scale(key, dims, pieces, -0.22, 0.18) * drawn
    return jnp.clip(drawn, min=-most, max=most).astype(kind)


def setup_inputs(seed: int = 0, part: int = 0) -> dict:
    streams_of = jax.random.split(jax.random.key(seed), 7)
    part_splits = jax.random.split(jax.random.fold_in(streams_of[6], part), 7)
    position = scatter_about(part_splits[0], (C, NX, NY, NZ), 1.0, 6.0, ((1, 32), (2, 4), (3, 2)), jnp.float32)
    momentum = scatter_about(part_splits[1], (C, NX, NY, NZ), 1.0, 6.0, ((1, 32), (2, 4), (3, 2)), jnp.float32)
    noise = scatter_about(part_splits[2], (STEPS, C, NX, NY, NZ), 1.0, 6.0, ((2, 32), (3, 4), (4, 2)))
    filter_in = scatter_about(streams_of[3], (C, C, 3, 3, 3), (27 * C) ** -0.5, 0.15625, ((0, 32), (1, 4)))
    filter_out = scatter_about(streams_of[4], (C, C, 3, 3, 3), (27 * C) ** -0.5, 0.15625, ((0, 32), (1, 4)))
    bias = scatter_about(streams_of[5], (C,), 1.0, 4.0, (), jnp.float32)
    return {"position": position, "momentum": momentum, "noise": noise, "filter_in": filter_in, "filter_out": filter_out, "bias": bias}


def convolve(field, filters):
    padded = jnp.pad(field, ((0, 0), (1, 1), (1, 1), (1, 1)), mode='wrap')
    return lax.conv_general_dilated(padded[None], filters, (1, 1, 1), 'VALID', dimension_numbers=('NCDHW', 'OIDHW', 'NCDHW'), preferred_element_type=jnp.float32)[0]

def adjoint(filters):
    return jnp.transpose(jnp.flip(filters, (2, 3, 4)), (1, 0, 2, 3, 4))

def reference(position, momentum, noise, filter_in, filter_out, bias):
    back_in = adjoint(filter_in)
    back_out = adjoint(filter_out)
    bias_col = bias[:, None, None, None]

    def gradient(field):
        rounded = field.astype(jnp.bfloat16)
        pre = convolve(rounded, filter_in) + bias_col
        active = jnp.tanh(pre)
        output = convolve(active.astype(jnp.bfloat16), filter_out)
        back = convolve(output.astype(jnp.bfloat16), back_out)
        hidden = (back * (1.0 - active * active)).astype(jnp.bfloat16)
        return convolve(hidden, back_in) + field
    step = 0.25
    decay = jnp.exp(jnp.float32(-0.25))
    kick = jnp.sqrt(1.0 - decay * decay)
    field = position
    moment = momentum
    force = gradient(field)
    for index in range(STEPS):
        moment = moment - 0.5 * step * force
        field = field + 0.5 * step * moment
        moment = decay * moment + kick * noise[index].astype(jnp.float32)
        field = field + 0.5 * step * moment
        force = gradient(field)
        moment = moment - 0.5 * step * force
    return (field, moment)
```

```python
import jax
import jax.numpy as jnp
from jax import lax
from jax.experimental import pallas as pl
from jax.experimental.pallas import tpu as pltpu
from jax.sharding import PartitionSpec as P

MESH = pl.DeviceIdType.MESH
EDGE = 16
AROUND = [(dx, dy) for dx in (-1, 1) for dy in (-1, 1)] + [(-1, 0), (1, 0), (0, -1), (0, 1)]


def shifted_sum(parts, slot, rows, count):
    low = pltpu.roll(parts[0, slot], 1, 0)
    high = pltpu.roll(parts[2, slot], rows - 1, 0)
    return low + parts[1, slot] + high


def kernel(
    position, momentum, noise, filters, adjoints, bias, out_position, out_momentum,
    wide_in, wide_out, slim_in, slim_out, band, outer, own, own_edge, back, back_edge,
    q, p, force, active, hidden, wide_parts, slim_parts, send_sem, recv_sem,
):
    steps = noise.shape[0]
    depth, lanes = own.shape[1:]
    half = lanes // 2
    rows = band.shape[2]
    gx, gy, gz = (lax.axis_index(name) for name in ("gx", "gy", "gz"))
    nx, ny, nz = (lax.axis_size(name) for name in ("gx", "gy", "gz"))
    partner = lax.rem(gz + 1, nz)

    def at(dx, dy, z):
        return {"gx": lax.rem(gx + dx + nx, nx), "gy": lax.rem(gy + dy + ny, ny), "gz": z}

    barrier = pltpu.get_barrier_semaphore()
    for dx, dy in AROUND:
        pl.semaphore_signal(barrier, inc=1, device_id=at(dx, dy, gz), device_id_type=MESH)
        pl.semaphore_signal(barrier, inc=1, device_id=at(dx, dy, partner), device_id_type=MESH)
    pl.semaphore_signal(barrier, inc=1, device_id=at(0, 0, partner), device_id_type=MESH)
    pl.semaphore_wait(barrier, 2 * len(AROUND) + 1)

    def copies(which, block, edge, padded):
        found = []
        for n, (dx, dy) in enumerate(AROUND):
            spot = padded.at[1 - dy, pl.ds(2 - 2 * dx, 2)]
            found.append(
                pltpu.make_async_remote_copy(
                    src_ref=block, dst_ref=spot.at[:, pl.ds(0, depth)],
                    send_sem=send_sem.at[which, 2 * n], recv_sem=recv_sem.at[which, 2 * n],
                    device_id=at(dx, dy, gz), device_id_type=MESH,
                )
            )
            found.append(
                pltpu.make_async_remote_copy(
                    src_ref=edge, dst_ref=spot.at[:, pl.ds(depth, EDGE)],
                    send_sem=send_sem.at[which, 2 * n + 1], recv_sem=recv_sem.at[which, 2 * n + 1],
                    device_id=at(dx, dy, partner), device_id_type=MESH,
                )
            )
        last = 2 * len(AROUND)
        found.append(
            pltpu.make_async_remote_copy(
                src_ref=edge, dst_ref=padded.at[1, pl.ds(2, 2), pl.ds(depth, EDGE)],
                send_sem=send_sem.at[which, last], recv_sem=recv_sem.at[which, last],
                device_id=at(0, 0, partner), device_id_type=MESH,
            )
        )
        return found

    def exchange(which, value, block, edge, padded):
        row = lax.broadcasted_iota(jnp.int32, (2, EDGE, lanes), 1)
        first = value[:, :EDGE].astype(jnp.float32)
        final = value[:, depth - EDGE :].astype(jnp.float32)
        block[...] = value
        edge[...] = jnp.where(row < EDGE // 2, first, final).astype(jnp.bfloat16)
        sent = copies(which, block, edge, padded)
        for copy in sent:
            copy.start()
        padded[1, 2:4, 0:depth] = value
        for copy in sent:
            copy.wait()

    def wide(padded, weights):
        @pl.loop(0, 3)
        def _(c):
            pieces = [
                padded[y, a : a + 4].reshape(4 * rows, lanes) for a in range(3) for y in range(3)
            ]
            made = jnp.dot(
                jnp.concatenate(pieces, axis=1), weights[c], preferred_element_type=jnp.float32
            )
            wide_parts[c] = made.reshape(4, rows, 2 * lanes)

    def slim(weights):
        pieces = [hidden[a : a + 2].reshape(2 * rows, 2 * lanes) for a in range(3)]
        taps = jnp.concatenate(pieces, axis=1)
        for c in range(3):
            made = jnp.dot(taps, weights[c], preferred_element_type=jnp.float32)
            slim_parts[c] = made.reshape(2, rows, lanes)

    def banded(source, which, target, wide_one):
        target[...] = jnp.zeros_like(target)
        span = 6 if wide_one else 4

        @pl.loop(0, 9)
        def _(tap):
            c, a = tap // 3, lax.rem(tap, 3)
            taps = [source[which, a, b, c] for b in range(3)]
            zero = jnp.zeros((half, half), jnp.bfloat16)
            pairs = [
                jnp.concatenate([taps[b] if b < 3 else zero, taps[b - 1] if b > 0 else zero], axis=1)
                for b in range(4)
            ]
            for group in range(2 if wide_one else 1):
                for b in range(4):
                    start = pl.multiple_of(a * (span * half) + (2 * group + b) * half, half)
                    target[c, pl.ds(start, half), group * lanes : (group + 1) * lanes] = pairs[b]

    banded(filters, 0, wide_in, True)
    banded(filters, 1, slim_out, False)
    banded(adjoints, 1, wide_out, True)
    banded(adjoints, 0, slim_in, False)

    for x in range(2):
        q[x] = position[x].T
        p[x] = momentum[x].T

    size = 0.25
    decay = jnp.exp(jnp.float32(-0.25))
    kick = jnp.sqrt(1.0 - decay * decay)

    @pl.loop(0, steps + 1)
    def _(k):
        exchange(0, q[...].astype(jnp.bfloat16), own, own_edge, band)
        wide(band, wide_in)
        for x in range(4):
            t = jnp.tanh(shifted_sum(wide_parts, x, rows, 4) + bias[...])
            active[x] = t
            hidden[x] = t.astype(jnp.bfloat16)
        slim(slim_out)
        out = [shifted_sum(slim_parts, x, rows, 2)[:depth].astype(jnp.bfloat16) for x in range(2)]
        exchange(1, jnp.stack(out), back, back_edge, outer)
        wide(outer, wide_out)
        for x in range(4):
            t = active[x]
            gu = shifted_sum(wide_parts, x, rows, 4)
            hidden[x] = (gu * (1.0 - t * t)).astype(jnp.bfloat16)
        slim(slim_in)
        for x in range(2):
            force[x] = shifted_sum(slim_parts, x, rows, 2)[:depth] + q[x]

        @pl.when(k > 0)
        def _():
            p[...] = p[...] - 0.5 * size * force[...]

        @pl.when(k < steps)
        def _():
            for x in range(2):
                drawn = noise[lax.min(k, steps - 1), x].astype(jnp.float32).T
                moment = p[x] - 0.5 * size * force[x]
                field = q[x] + 0.5 * size * moment
                moment = decay * moment + kick * drawn
                q[x] = field + 0.5 * size * moment
                p[x] = moment

    for x in range(2):
        out_position[x] = q[x].T
        out_momentum[x] = p[x].T


def on_device(position, momentum, noise, filter_in, filter_out, bias):
    channels, nx, ny, depth = position.shape
    steps = noise.shape[0]
    lanes = ny * channels
    rows = depth + EDGE

    own = jnp.stack([filter_in, filter_out])
    two, o_own, i_own = own.shape[:3]
    flat = own.reshape(two, o_own, i_own, 27)
    every = lax.all_gather(flat, ("gx", "gy"), axis=0)
    parts_x, parts_y = lax.axis_size("gx"), lax.axis_size("gy")
    every = every.reshape(parts_x, parts_y, two, o_own, i_own, 27)
    natural = jnp.transpose(every, (2, 5, 0, 3, 1, 4)).reshape(two, 3, 3, 3, channels, channels)
    adjoints = jnp.flip(natural, (1, 2, 3))
    filters = jnp.swapaxes(natural, -1, -2)

    def to_planes(block):
        return jnp.transpose(block, (1, 2, 0, 3)).reshape(nx, lanes, depth)

    def from_planes(planes):
        return jnp.transpose(planes.reshape(nx, ny, channels, depth), (2, 0, 1, 3))

    noise_planes = jnp.transpose(noise, (0, 2, 3, 1, 4)).reshape(steps, nx, lanes, depth)
    bias_row = jnp.tile(bias, 2 * ny).reshape(1, 2 * lanes)

    bf, f32 = jnp.bfloat16, jnp.float32
    messages = 2 * len(AROUND) + 1
    planes = jax.ShapeDtypeStruct((nx, lanes, depth), f32)
    vmem = pl.BlockSpec(memory_space=pltpu.VMEM)
    final_position, final_momentum = pl.pallas_call(
        kernel,
        out_shape=(planes, planes),
        in_specs=[vmem] * 6,
        out_specs=(vmem, vmem),
        scratch_shapes=[
            pltpu.VMEM((3, 9 * lanes, 2 * lanes), bf),
            pltpu.VMEM((3, 9 * lanes, 2 * lanes), bf),
            pltpu.VMEM((3, 6 * lanes, lanes), bf),
            pltpu.VMEM((3, 6 * lanes, lanes), bf),
            pltpu.VMEM((3, 6, rows, lanes), bf),
            pltpu.VMEM((3, 6, rows, lanes), bf),
            pltpu.VMEM((nx, depth, lanes), bf),
            pltpu.VMEM((nx, EDGE, lanes), bf),
            pltpu.VMEM((nx, depth, lanes), bf),
            pltpu.VMEM((nx, EDGE, lanes), bf),
            pltpu.VMEM((nx, depth, lanes), f32),
            pltpu.VMEM((nx, depth, lanes), f32),
            pltpu.VMEM((nx, depth, lanes), f32),
            pltpu.VMEM((4, rows, 2 * lanes), f32),
            pltpu.VMEM((4, rows, 2 * lanes), bf),
            pltpu.VMEM((3, 4, rows, 2 * lanes), f32),
            pltpu.VMEM((3, 2, rows, lanes), f32),
            pltpu.SemaphoreType.DMA((2, messages)),
            pltpu.SemaphoreType.DMA((2, messages)),
        ],
        compiler_params=pltpu.CompilerParams(
            collective_id=0, has_side_effects=True, vmem_limit_bytes=40 * 1024 * 1024
        ),
        name="langevin",
    )(to_planes(position), to_planes(momentum), noise_planes, filters, adjoints, bias_row)
    return from_planes(final_position), from_planes(final_momentum)


def solution(mesh):
    field = P(None, ("grp", "gx"), "gy", "gz")
    in_specs = (
        field,
        field,
        P(None, None, ("grp", "gx"), "gy", "gz"),
        P("gx", "gy", None, None, None),
        P("gx", "gy", None, None, None),
        P(),
    )
    return jax.shard_map(
        on_device, mesh=mesh, in_specs=in_specs, out_specs=(field, field), check_vma=False
    )
```

```python
import jax
import jax.numpy as jnp
from jax import lax
from jax.experimental import pallas as pl
from jax.experimental.pallas import tpu as pltpu
from jax.sharding import PartitionSpec as P

MESH = pl.DeviceIdType.MESH
EDGE = 16
AROUND = [(dx, dy) for dx in (-1, 1) for dy in (-1, 1)] + [(-1, 0), (1, 0), (0, -1), (0, 1)]


def shifted_sum(parts, slot, rows, count):
    low = pltpu.roll(parts[0, slot], 1, 0)
    high = pltpu.roll(parts[2, slot], rows - 1, 0)
    return low + parts[1, slot] + high


def kernel(
    position, momentum, noise, filters, adjoints, bias, out_position, out_momentum,
    wide_in, wide_out, slim_in, slim_out, band, outer, own, own_edge, back, back_edge,
    q, p, force, active, hidden, wide_parts, slim_parts, send_sem, recv_sem,
):
    steps = noise.shape[0]
    depth, lanes = own.shape[1:]
    half = lanes // 2
    rows = band.shape[2]
    gx, gy, gz = (lax.axis_index(name) for name in ("gx", "gy", "gz"))
    nx, ny, nz = (lax.axis_size(name) for name in ("gx", "gy", "gz"))
    partner = lax.rem(gz + 1, nz)

    def at(dx, dy, z):
        return {"gx": lax.rem(gx + dx + nx, nx), "gy": lax.rem(gy + dy + ny, ny), "gz": z}

    barrier = pltpu.get_barrier_semaphore()
    for dx, dy in AROUND:
        pl.semaphore_signal(barrier, inc=1, device_id=at(dx, dy, gz), device_id_type=MESH)
        pl.semaphore_signal(barrier, inc=1, device_id=at(dx, dy, partner), device_id_type=MESH)
    pl.semaphore_signal(barrier, inc=1, device_id=at(0, 0, partner), device_id_type=MESH)
    pl.semaphore_wait(barrier, 2 * len(AROUND) + 1)

    def copies(which, block, edge, padded):
        found = []
        for n, (dx, dy) in enumerate(AROUND):
            spot = padded.at[1 - dy, pl.ds(2 - 2 * dx, 2)]
            found.append(
                pltpu.make_async_remote_copy(
                    src_ref=block, dst_ref=spot.at[:, pl.ds(0, depth)],
                    send_sem=send_sem.at[which, 2 * n], recv_sem=recv_sem.at[which, 2 * n],
                    device_id=at(dx, dy, gz), device_id_type=MESH,
                )
            )
            found.append(
                pltpu.make_async_remote_copy(
                    src_ref=edge, dst_ref=spot.at[:, pl.ds(depth, EDGE)],
                    send_sem=send_sem.at[which, 2 * n + 1], recv_sem=recv_sem.at[which, 2 * n + 1],
                    device_id=at(dx, dy, partner), device_id_type=MESH,
                )
            )
        last = 2 * len(AROUND)
        found.append(
            pltpu.make_async_remote_copy(
                src_ref=edge, dst_ref=padded.at[1, pl.ds(2, 2), pl.ds(depth, EDGE)],
                send_sem=send_sem.at[which, last], recv_sem=recv_sem.at[which, last],
                device_id=at(0, 0, partner), device_id_type=MESH,
            )
        )
        return found

    def exchange(which, value, block, edge, padded):
        row = lax.broadcasted_iota(jnp.int32, (2, EDGE, lanes), 1)
        first = value[:, :EDGE].astype(jnp.float32)
        final = value[:, depth - EDGE :].astype(jnp.float32)
        block[...] = value
        edge[...] = jnp.where(row < EDGE // 2, first, final).astype(jnp.bfloat16)
        sent = copies(which, block, edge, padded)
        for copy in sent:
            copy.start()
        padded[1, 2:4, 0:depth] = value
        for copy in sent:
            copy.wait()

    def wide(padded, weights):
        @pl.loop(0, 3)
        def _(c):
            pieces = [
                padded[y, a : a + 4].reshape(4 * rows, lanes) for a in range(3) for y in range(3)
            ]
            made = jnp.dot(
                jnp.concatenate(pieces, axis=1), weights[c], preferred_element_type=jnp.float32
            )
            wide_parts[c] = made.reshape(4, rows, 2 * lanes)

    def slim(weights):
        pieces = [hidden[a : a + 2].reshape(2 * rows, 2 * lanes) for a in range(3)]
        taps = jnp.concatenate(pieces, axis=1)
        for c in range(3):
            made = jnp.dot(taps, weights[c], preferred_element_type=jnp.float32)
            slim_parts[c] = made.reshape(2, rows, lanes)

    def banded(source, which, target, wide_one, flipped):
        target[...] = jnp.zeros_like(target)
        span = 6 if wide_one else 4

        @pl.loop(0, 9)
        def _(tap):
            c, a = tap // 3, lax.rem(tap, 3)
            taps = [
                source[which, 2 - a, 2 - b, 2 - c] if flipped else source[which, a, b, c]
                for b in range(3)
            ]
            zero = jnp.zeros((half, half), jnp.bfloat16)
            pairs = [
                jnp.concatenate([taps[b] if b < 3 else zero, taps[b - 1] if b > 0 else zero], axis=1)
                for b in range(4)
            ]
            for group in range(2 if wide_one else 1):
                for b in range(4):
                    start = pl.multiple_of(a * (span * half) + (2 * group + b) * half, half)
                    target[c, pl.ds(start, half), group * lanes : (group + 1) * lanes] = pairs[b]

    banded(filters, 0, wide_in, True, False)
    banded(filters, 1, slim_out, False, False)
    banded(adjoints, 1, wide_out, True, True)
    banded(adjoints, 0, slim_in, False, True)

    for x in range(2):
        q[x] = position[x].T
        p[x] = momentum[x].T

    size = 0.25
    decay = jnp.exp(jnp.float32(-0.25))
    kick = jnp.sqrt(1.0 - decay * decay)

    @pl.loop(0, steps + 1)
    def _(k):
        exchange(0, q[...].astype(jnp.bfloat16), own, own_edge, band)
        wide(band, wide_in)
        for x in range(4):
            t = jnp.tanh(shifted_sum(wide_parts, x, rows, 4) + bias[...])
            active[x] = t
            hidden[x] = t.astype(jnp.bfloat16)
        slim(slim_out)
        out = [shifted_sum(slim_parts, x, rows, 2)[:depth].astype(jnp.bfloat16) for x in range(2)]
        exchange(1, jnp.stack(out), back, back_edge, outer)
        wide(outer, wide_out)
        for x in range(4):
            t = active[x]
            gu = shifted_sum(wide_parts, x, rows, 4)
            hidden[x] = (gu * (1.0 - t * t)).astype(jnp.bfloat16)
        slim(slim_in)
        for x in range(2):
            force[x] = shifted_sum(slim_parts, x, rows, 2)[:depth] + q[x]

        @pl.when(k > 0)
        def _():
            p[...] = p[...] - 0.5 * size * force[...]

        @pl.when(k < steps)
        def _():
            for x in range(2):
                drawn = noise[lax.min(k, steps - 1), x].astype(jnp.float32).T
                moment = p[x] - 0.5 * size * force[x]
                field = q[x] + 0.5 * size * moment
                moment = decay * moment + kick * drawn
                q[x] = field + 0.5 * size * moment
                p[x] = moment

    for x in range(2):
        out_position[x] = q[x].T
        out_momentum[x] = p[x].T


def gather_kernel(piece, every, line_send, line_recv, send_sem, recv_sem, own_sem):
    gx, gy = lax.axis_index("gx"), lax.axis_index("gy")
    nx, ny = lax.axis_size("gx"), lax.axis_size("gy")
    right, left = lax.rem(gx + 1, nx), lax.rem(gx + nx - 1, nx)
    barrier = pltpu.get_barrier_semaphore()
    for j in range(1, ny):
        pl.semaphore_signal(barrier, inc=1, device_id={"gy": lax.rem(gy + j, ny)}, device_id_type=MESH)
    for x in (left, right):
        pl.semaphore_signal(barrier, inc=1, device_id={"gx": x}, device_id_type=MESH)
    pl.semaphore_wait(barrier, ny + 1)

    line = [
        pltpu.make_async_remote_copy(
            src_ref=piece, dst_ref=every.at[gx, gy],
            send_sem=line_send.at[j], recv_sem=line_recv.at[j],
            device_id={"gy": lax.rem(gy + j, ny)}, device_id_type=MESH,
        )
        for j in range(1, ny)
    ]
    line.append(pltpu.make_async_copy(piece, every.at[gx, gy], own_sem))
    for copy in line:
        copy.start()
    for copy in line:
        copy.wait()

    def passed(way, step):
        owner = lax.rem(gx - step + nx, nx) if way == 0 else lax.rem(gx + step, nx)
        return pltpu.make_async_remote_copy(
            src_ref=every.at[owner], dst_ref=every.at[owner],
            send_sem=send_sem.at[way, step], recv_sem=recv_sem.at[way, step],
            device_id={"gx": right if way == 0 else left}, device_id_type=MESH,
        )

    both = (nx - 1) // 2

    @pl.loop(0, both)
    def _(step):
        copies = [passed(way, step) for way in range(2)]
        for copy in copies:
            copy.start()
        for copy in copies:
            copy.wait()

    if nx % 2 == 0:
        copy = passed(0, both)
        copy.start()
        copy.wait()


def gathered(piece):
    nx, ny = lax.axis_size("gx"), lax.axis_size("gy")
    vmem = pl.BlockSpec(memory_space=pltpu.VMEM)
    return pl.pallas_call(
        gather_kernel,
        out_shape=jax.ShapeDtypeStruct((nx, ny, *piece.shape), piece.dtype),
        in_specs=[vmem],
        out_specs=vmem,
        scratch_shapes=[
            pltpu.SemaphoreType.DMA((ny,)),
            pltpu.SemaphoreType.DMA((ny,)),
            pltpu.SemaphoreType.DMA((2, nx // 2)),
            pltpu.SemaphoreType.DMA((2, nx // 2)),
            pltpu.SemaphoreType.DMA,
        ],
        compiler_params=pltpu.CompilerParams(collective_id=1, has_side_effects=True),
        name="gather",
    )(piece)


def on_device(position, momentum, noise, filter_in, filter_out, bias):
    channels, nx, ny, depth = position.shape
    steps = noise.shape[0]
    lanes = ny * channels
    rows = depth + EDGE

    own = jnp.stack([filter_in, filter_out])
    two, o_own, i_own = own.shape[:3]
    taps_first = jnp.transpose(own.reshape(two, o_own, i_own, 27), (3, 0, 1, 2)).reshape(27, -1)
    spare = -27 % (16 * 128 // taps_first.shape[1])
    piece = jnp.pad(taps_first, ((0, spare), (0, 0))).reshape(-1, 128)
    parts_x, parts_y = lax.axis_size("gx"), lax.axis_size("gy")
    every = gathered(piece).reshape(parts_x, parts_y, 27 + spare, two, o_own, i_own)[:, :, :27]
    adjoints = jnp.transpose(every, (3, 2, 0, 4, 1, 5)).reshape(two, 3, 3, 3, channels, channels)
    filters = jnp.swapaxes(adjoints, -1, -2)

    def to_planes(block):
        return jnp.transpose(block, (1, 2, 0, 3)).reshape(nx, lanes, depth)

    def from_planes(planes):
        return jnp.transpose(planes.reshape(nx, ny, channels, depth), (2, 0, 1, 3))

    noise_planes = jnp.transpose(noise, (0, 2, 3, 1, 4)).reshape(steps, nx, lanes, depth)
    bias_row = jnp.tile(bias, 2 * ny).reshape(1, 2 * lanes)

    bf, f32 = jnp.bfloat16, jnp.float32
    messages = 2 * len(AROUND) + 1
    planes = jax.ShapeDtypeStruct((nx, lanes, depth), f32)
    vmem = pl.BlockSpec(memory_space=pltpu.VMEM)
    final_position, final_momentum = pl.pallas_call(
        kernel,
        out_shape=(planes, planes),
        in_specs=[vmem] * 6,
        out_specs=(vmem, vmem),
        scratch_shapes=[
            pltpu.VMEM((3, 9 * lanes, 2 * lanes), bf),
            pltpu.VMEM((3, 9 * lanes, 2 * lanes), bf),
            pltpu.VMEM((3, 6 * lanes, lanes), bf),
            pltpu.VMEM((3, 6 * lanes, lanes), bf),
            pltpu.VMEM((3, 6, rows, lanes), bf),
            pltpu.VMEM((3, 6, rows, lanes), bf),
            pltpu.VMEM((nx, depth, lanes), bf),
            pltpu.VMEM((nx, EDGE, lanes), bf),
            pltpu.VMEM((nx, depth, lanes), bf),
            pltpu.VMEM((nx, EDGE, lanes), bf),
            pltpu.VMEM((nx, depth, lanes), f32),
            pltpu.VMEM((nx, depth, lanes), f32),
            pltpu.VMEM((nx, depth, lanes), f32),
            pltpu.VMEM((4, rows, 2 * lanes), f32),
            pltpu.VMEM((4, rows, 2 * lanes), bf),
            pltpu.VMEM((3, 4, rows, 2 * lanes), f32),
            pltpu.VMEM((3, 2, rows, lanes), f32),
            pltpu.SemaphoreType.DMA((2, messages)),
            pltpu.SemaphoreType.DMA((2, messages)),
        ],
        compiler_params=pltpu.CompilerParams(
            collective_id=0, has_side_effects=True, vmem_limit_bytes=40 * 1024 * 1024
        ),
        name="langevin",
    )(to_planes(position), to_planes(momentum), noise_planes, filters, adjoints, bias_row)
    return from_planes(final_position), from_planes(final_momentum)


def solution(mesh):
    field = P(None, ("grp", "gx"), "gy", "gz")
    in_specs = (
        field,
        field,
        P(None, None, ("grp", "gx"), "gy", "gz"),
        P("gx", "gy", None, None, None),
        P("gx", "gy", None, None, None),
        P(),
    )
    return jax.shard_map(
        on_device, mesh=mesh, in_specs=in_specs, out_specs=(field, field), check_vma=False
    )
```
